256 devices in a mesh: ctx: 32 (over z, y), head: 8 (over x, core).
Axes of the slice: x: 4, y: 4, z: 8, core: 2. Of those that a mesh axis runs over, the one named last changes fastest.
Arguments:
- queries: bfloat16 [64, 32768, 128], P('head', 'ctx'), may hold values from -54.5 to 54.5
- key_heads: bfloat16 [8, 32768, 128], P('head', 'ctx'), may hold values from -6.8125 to 6.8125
- value_tensor: bfloat16 [8, 32768, 128], P('head', 'ctx'), may hold values from -6 to 6
- distance_use: int32 [32, 5], P('ctx'), may hold values 0 or 1
- block_pick: int32 [256, 5], P('ctx'), may hold values from 0 to 7
Outputs:
- attended: bfloat16 [64, 32768, 128], P(None, ('ctx', 'head'))
The draws below stay inside these ranges and needn't reach their ends.
All inputs are finite; a program needn't handle non-finite values. No bound on the sum of `distance_use` on one device may be relied on, other than what follows from the above.
Results may differ from the reference program's by a relative error of at most 0.0029.
Values may be sent and summed in bfloat16 or wider, within the bound.
A program may use at most 64 MiB of HBM per device.

```python
import math
import jax
import jax.numpy as jnp
from jax import lax

QUERY_HEADS = 64
KEY_VALUE_HEADS = 8
HEAD_SIZE = 128
SHARD_TOKENS = 1024
BLOCK_TOKENS = 128
SHARDS = 32
PARTNER_STEPS = 5
SEQUENCE_TOKENS = 32768
N_CTX = 32


def query_key_common(key):
    query_seed, random_key_seed = jax.random.split(jax.random.fold_in(key, 7))
    partner_offset = 1.7
    key_entries = jnp.clip(jax.random.normal(random_key_seed, (KEY_VALUE_HEADS, SEQUENCE_TOKENS, HEAD_SIZE), jnp.float32) * partner_offset, -4.0 * partner_offset, 4.0 * partner_offset)
    query_vals = jnp.clip(jax.random.normal(query_seed, (QUERY_HEADS, SEQUENCE_TOKENS, HEAD_SIZE), jnp.float32) * partner_offset, -4.0 * partner_offset, 4.0 * partner_offset)
    return (query_vals, key_entries)


def draw_queries(key, part):
    return query_key_common(key)[0].astype(jnp.bfloat16)


def draw_key_heads(key, part):
    return query_key_common(key)[1].astype(jnp.bfloat16)


def set_ends(values, stream_key, smallest, largest):
    longest = values.shape.index(max(values.shape))
    spots = []
    for shift in (0, 1):
        where = [jax.random.randint(jax.random.fold_in(stream_key, axis), (), 0, length) for axis, length in enumerate(values.shape)]
        where[longest] = (where[longest] + shift) % values.shape[longest]
        spots.append(tuple(where))
    return values.at[spots[0]].set(smallest).at[spots[1]].set(largest)


def block_levels(key, dims, cuts, least, largest):
    def one(axis_at, parts):
        heights = jax.random.uniform(jax.random.fold_in(jax.random.fold_in(key, 6), axis_at), (parts,), jnp.float32, least / len(cuts), largest / len(cuts))
        return jnp.repeat(jnp.exp(heights), dims[axis_at] // parts).reshape((-1,) + (1,) * (len(dims) - axis_at - 1))

    gain = one(*cuts[0])
    for cut in cuts[1:]:
        gain = gain * one(*cut)
    return gain


def bell_draw(own_key, extent, spread, most, shards=(), kind=jnp.bfloat16):
    factor_of = block_levels(own_key, extent, shards, -0.22, 0.18) if shards else 1.0
    values = jax.random.normal(own_key, extent, jnp.float32) * spread * factor_of
    return jnp.minimum(jnp.maximum(values, -most), most).astype(kind)


def setup_inputs(seed: int = 0) -> dict:
    key_list = jax.random.split(jax.random.key(seed), 6)
    return {
        "queries": draw_queries(jax.random.fold_in(key_list[5], 71), 0),
        "key_heads": draw_key_heads(jax.random.fold_in(key_list[5], 71), 0),
        "value_tensor": bell_draw(key_list[2], (KEY_VALUE_HEADS, SEQUENCE_TOKENS, HEAD_SIZE), 1.0, 6.0, ((0, 8), (1, 32))),
        "distance_use": set_ends((jax.random.randint(key_list[3], (SHARDS, PARTNER_STEPS), 0, 4) < 3).astype(jnp.int32), jax.random.fold_in(key_list[3], 1), 0, 1),
        "block_pick": set_ends(jax.random.randint(key_list[4], (SEQUENCE_TOKENS // BLOCK_TOKENS, PARTNER_STEPS), 0, SHARD_TOKENS // BLOCK_TOKENS), jax.random.fold_in(key_list[4], 1), 0, (SHARD_TOKENS // BLOCK_TOKENS) - 1).astype(jnp.int32),
    }


def reference(queries, key_heads, value_tensor, distance_use, block_pick):
    number_of_blocks = SHARD_TOKENS // BLOCK_TOKENS
    query_group_width = QUERY_HEADS // KEY_VALUE_HEADS
    score_scale = 1.0 / math.sqrt(HEAD_SIZE)
    strides = jnp.array([2 ** step_index for step_index in range(PARTNER_STEPS)], jnp.int32)
    offsets = jnp.arange(BLOCK_TOKENS, dtype=jnp.int32)
    row_pos = lax.broadcasted_iota(jnp.int32, (SHARD_TOKENS, SHARD_TOKENS), 0)
    col_pos = lax.broadcasted_iota(jnp.int32, (SHARD_TOKENS, SHARD_TOKENS), 1)
    causal = col_pos <= row_pos

    def single_partner(partner_index):
        shard_slice = partner_index // KEY_VALUE_HEADS
        key_value_index = partner_index % KEY_VALUE_HEADS
        start = shard_slice * SHARD_TOKENS
        query_matrix = lax.dynamic_slice(queries, (key_value_index * query_group_width, start, jnp.int32(0)), (query_group_width, SHARD_TOKENS, HEAD_SIZE)).astype(jnp.float32)
        key_all = lax.dynamic_index_in_dim(key_heads, key_value_index, 0, False)
        value_all = lax.dynamic_index_in_dim(value_tensor, key_value_index, 0, False)
        key_local = lax.dynamic_slice_in_dim(key_all, start, SHARD_TOKENS, 0).astype(jnp.float32)
        value_local = lax.dynamic_slice_in_dim(value_all, start, SHARD_TOKENS, 0).astype(jnp.float32)
        picks = lax.dynamic_slice_in_dim(block_pick, shard_slice * number_of_blocks, number_of_blocks, 0)
        source = shard_slice - strides
        live = (lax.dynamic_index_in_dim(distance_use, shard_slice, 0, False) == 1) & (source >= 0)
        rows_index = (jnp.maximum(source, 0)[None, :, None] * SHARD_TOKENS + picks[:, :, None] * BLOCK_TOKENS + offsets[None, None, :]).reshape(number_of_blocks, PARTNER_STEPS * BLOCK_TOKENS).astype(jnp.int32)
        remote_key = key_all[rows_index].astype(jnp.float32)
        remote_value = value_all[rows_index].astype(jnp.float32)
        far_live = jnp.repeat(live, BLOCK_TOKENS)
        near_scores = jnp.einsum('hqd,kd->hqk', query_matrix, key_local) * score_scale
        near_scores = jnp.where(causal[None], near_scores, -jnp.inf)
        remote_scores = jnp.einsum('ogfc,gic->ogfi', query_matrix.reshape(query_group_width, number_of_blocks, BLOCK_TOKENS, HEAD_SIZE), remote_key) * score_scale
        remote_scores = jnp.where(far_live[None, None, None, :], remote_scores, -jnp.inf)
        remote_scores = remote_scores.reshape(query_group_width, SHARD_TOKENS, PARTNER_STEPS * BLOCK_TOKENS)
        row_peak = jnp.maximum(lax.optimization_barrier(jnp.max(near_scores, axis=-1, keepdims=True)), lax.optimization_barrier(jnp.max(remote_scores, axis=-1, keepdims=True)))
        near_weights = jnp.exp(near_scores - row_peak)
        far_weights = jnp.exp(remote_scores - row_peak)
        row_total = lax.optimization_barrier(jnp.sum(near_weights, axis=-1, keepdims=True)) + lax.optimization_barrier(jnp.sum(far_weights, axis=-1, keepdims=True))
        rounded_near = lax.optimization_barrier(near_weights.astype(jnp.bfloat16)).astype(jnp.float32)
        remote_rounded = lax.optimization_barrier(far_weights.astype(jnp.bfloat16)).astype(jnp.float32)
        running_sum = jnp.einsum('hqk,kd->hqd', rounded_near, value_local)
        running_sum = running_sum + jnp.einsum('vltf,lfe->vlte', remote_rounded.reshape(query_group_width, number_of_blocks, BLOCK_TOKENS, PARTNER_STEPS * BLOCK_TOKENS), remote_value).reshape(query_group_width, SHARD_TOKENS, HEAD_SIZE)
        return (running_sum / row_total).astype(jnp.bfloat16)
    output_list = lax.map(single_partner, jnp.arange(N_CTX * KEY_VALUE_HEADS, dtype=jnp.int32))
    output_list = output_list.reshape(N_CTX, KEY_VALUE_HEADS, query_group_width, SHARD_TOKENS, HEAD_SIZE)
    return jnp.transpose(output_list, (1, 2, 0, 3, 4)).reshape(QUERY_HEADS, N_CTX * SHARD_TOKENS, HEAD_SIZE)
```

```python
import functools
import math

import jax
import jax.numpy as jnp
from jax import lax
from jax.experimental import pallas as pl
from jax.experimental.pallas import tpu as pltpu
from jax.sharding import PartitionSpec as P

BLOCK = 128
LEVELS = 5
Y_COUNT = 4
FORWARD_BLOCKS = 3
Y1, Y2, Z1, Z2, Z4F, RELAY, Z4B = range(7)
EXCHANGE_ORDER = (4, 3, 5, 2, 6, 1, 7)


def kernel(
    q_hbm, k_ref, v_ref, use_ref, pick_ref, out_ref,
    q_ref, far_keys, far_values, relay_ref, total_ref, inverse_ref, weight_ref, made_ref,
    send_sem, recv_sem, out_send_sem, out_recv_sem, own_sem,
):
    heads, tokens, width = q_ref.shape
    blocks = tokens // BLOCK
    ctx = lax.axis_index("ctx")
    head = lax.axis_index("head")
    shards = lax.axis_size("ctx")
    head_devices = lax.axis_size("head")
    z = ctx // Y_COUNT
    y = ctx % Y_COUNT
    along_z = lambda steps: lax.rem(ctx + (steps * Y_COUNT) % shards, shards)
    along_y = lambda steps: z * Y_COUNT + lax.rem(y + steps % Y_COUNT, Y_COUNT)

    take_queries = pltpu.make_async_copy(q_hbm, q_ref, own_sem.at[0])
    take_queries.start()

    barrier = pltpu.get_barrier_semaphore()
    ctx_peers = [along_z(s) for s in (1, -1, 2, -2, 3, -3)] + [along_y(s) for s in (1, -1, 2)]
    for peer in ctx_peers:
        pl.semaphore_signal(barrier, inc=1, device_id={"ctx": peer}, device_id_type=pl.DeviceIdType.MESH)
    for step in range(1, head_devices):
        pl.semaphore_signal(
            barrier, inc=1, device_id={"head": lax.rem(head + step, head_devices)},
            device_id_type=pl.DeviceIdType.MESH,
        )
    pl.semaphore_wait(barrier, len(ctx_peers) + head_devices - 1)

    own = (k_ref.at[0], v_ref.at[0])
    far = (far_keys, far_values)
    top = pl.ds(0, FORWARD_BLOCKS)
    rest = pl.ds(FORWARD_BLOCKS, blocks - FORWARD_BLOCKS)

    def copy(kind, lane, source, target, peer):
        return pltpu.make_async_remote_copy(
            src_ref=source, dst_ref=target,
            send_sem=send_sem.at[kind, lane], recv_sem=recv_sem.at[kind, lane],
            device_id={"ctx": peer}, device_id_type=pl.DeviceIdType.MESH,
        )

    def near_y1(t): return copy(t, Y1, own[t], far[t].at[0], along_y(1))
    def wrap_y1(t): return copy(t, Y1, far[t].at[2], far[t].at[0], along_y(1))
    def near_y2(t): return copy(t, Y2, own[t], far[t].at[1], along_y(2))
    def wrap_y2(t): return copy(t, Y2, far[t].at[2], far[t].at[1], along_y(2))
    def hop_z1(t): return copy(t, Z1, own[t], far[t].at[2], along_z(1))
    def hop_z2(t): return copy(t, Z2, far[t].at[2], far[t].at[3], along_z(1))
    def hop_z4f(t): return copy(t, Z4F, far[t].at[3, top], far[t].at[4, top], along_z(2))
    def hop_relay(t): return copy(t, RELAY, own[t].at[rest], relay_ref.at[t], along_z(-3))
    def hop_z4b(t): return copy(t, Z4B, relay_ref.at[t], far[t].at[4, rest], along_z(-1))

    relays = (z >= 5) | (z == 0)
    forwards = (z >= 2) & (z <= 5)

    def first(t):
        pl.when(z < 7)(lambda: hop_z1(t).start())
        pl.when(z < 4)(lambda: hop_relay(t).start())
        pl.when(y < 3)(lambda: near_y1(t).start())
        pl.when(y < 2)(lambda: near_y2(t).start())

    def second(t):
        @pl.when(z >= 1)
        def _():
            hop_z1(t).wait_recv()
            pl.when(z <= 6)(lambda: hop_z2(t).start())
            pl.when(y == 3)(lambda: wrap_y1(t).start())
            pl.when(y >= 2)(lambda: wrap_y2(t).start())

    def third(t):
        pl.when(z >= 2)(lambda: hop_z2(t).wait_recv())
        pl.when(forwards)(lambda: hop_z4f(t).start())

    def fourth(t):
        @pl.when(relays)
        def _():
            hop_relay(t).wait_recv()
            hop_z4b(t).start()

    def last(t):
        pl.when(ctx >= 1)(lambda: near_y1(t).wait_recv())
        pl.when(ctx >= 2)(lambda: near_y2(t).wait_recv())

        @pl.when(z >= 4)
        def _():
            hop_z4f(t).wait_recv()
            hop_z4b(t).wait_recv()

    def all_sent(t):
        pl.when(z < 7)(lambda: hop_z1(t).wait_send())
        pl.when(z < 4)(lambda: hop_relay(t).wait_send())
        pl.when((y < 3) | (z >= 1))(lambda: near_y1(t).wait_send())
        pl.when((y < 2) | (z >= 1))(lambda: near_y2(t).wait_send())
        pl.when((z >= 1) & (z <= 6))(lambda: hop_z2(t).wait_send())
        pl.when(forwards)(lambda: hop_z4f(t).wait_send())
        pl.when(relays)(lambda: hop_z4b(t).wait_send())

    first(0)
    for level in range(LEVELS):
        @pl.when(ctx < 2**level)
        def _(level=level):
            nothing = jnp.zeros((blocks, BLOCK, width), far_keys.dtype)
            far_keys[level] = nothing
            far_values[level] = nothing

    take_queries.wait()
    second(0)
    third(0)
    fourth(0)
    first(1)
    last(0)

    def picked(t, block):
        return jnp.concatenate(
            [far[t][level, pick_ref[block, level]] for level in range(LEVELS)], axis=0
        )

    exponent_scale = math.log2(math.e) / math.sqrt(width)
    bias = []
    for level in range(LEVELS):
        live = use_ref[0, level] * jnp.where(ctx >= 2**level, 1, 0)
        bias.append(jnp.full((1, BLOCK), (live.astype(jnp.float32) - 1.0) * 3e38, jnp.float32))
    bias = jnp.concatenate(bias, axis=1)
    rows = 2 * BLOCK

    def score_group(group):
        before = group * 2 * BLOCK
        near_width = before + 2 * BLOCK

        def body(step, carry):
            in_group = step // 4
            block = group * 2 + in_group
            pair = step % 4
            first_row = pl.multiple_of(block * BLOCK, BLOCK)
            row_slice = pl.ds(pl.multiple_of(pair * rows, rows), rows)
            q_now = q_ref[pl.ds(pair * 2, 2), pl.ds(first_row, BLOCK), :].reshape(rows, width)
            keys = jnp.concatenate([k_ref[0, : near_width // BLOCK].reshape(near_width, width), picked(0, block)], axis=0)
            scores = lax.dot_general(
                q_now, keys, (((1,), (1,)), ((), ())), preferred_element_type=jnp.float32
            )
            row_pos = lax.broadcasted_iota(jnp.int32, (rows, rows), 0) % BLOCK + in_group * BLOCK
            col_pos = lax.broadcasted_iota(jnp.int32, (rows, rows), 1)
            diagonal = jnp.where(col_pos <= row_pos, scores[:, before:near_width], -jnp.inf)
            distant = scores[:, near_width:] + bias
            parts = [scores[:, :before]] if group else []
            scores = jnp.concatenate(parts + [diagonal, distant], axis=1)
            peak = jnp.max(scores, axis=1, keepdims=True)
            weights = jnp.exp2((scores - peak) * exponent_scale)
            row_total = jnp.sum(weights, axis=1, keepdims=True)
            rounded = weights.astype(jnp.bfloat16)
            weight_ref[block, row_slice, :] = rounded[:, near_width:]
            total_ref[block, row_slice, :] = jnp.dot(
                rounded[:, :near_width], v_ref[0, : near_width // BLOCK].reshape(near_width, width), preferred_element_type=jnp.float32
            )
            inverse_ref[block, row_slice, :] = jnp.broadcast_to(1.0 / row_total, (rows, width))
            return carry

        lax.fori_loop(0, 8, body, 0)

    score_group(0)
    second(1)
    score_group(1)
    score_group(2)
    third(1)
    fourth(1)
    score_group(3)
    last(1)

    mine = pl.ds(head * heads, heads)

    def make(step):
        block = lax.rem(head + step, head_devices)
        values = picked(1, block)

        def body(pair, carry):
            row_slice = pl.ds(pl.multiple_of(pair * rows, rows), rows)
            distant = jnp.dot(weight_ref[block, row_slice, :], values, preferred_element_type=jnp.float32)
            result = (total_ref[block, row_slice, :] + distant) * inverse_ref[block, row_slice, :]
            made_ref[step, pl.ds(pair * 2, 2)] = result.astype(made_ref.dtype).reshape(2, BLOCK, width)
            return carry

        lax.fori_loop(0, heads // 2, body, 0)

    def give(step):
        return pltpu.make_async_remote_copy(
            src_ref=made_ref.at[step], dst_ref=out_ref.at[mine],
            send_sem=out_send_sem.at[step], recv_sem=out_recv_sem.at[step],
            device_id={"head": lax.rem(head + step, head_devices)},
            device_id_type=pl.DeviceIdType.MESH,
        )

    for place, step in enumerate(EXCHANGE_ORDER):
        make(step)
        if place:
            give(EXCHANGE_ORDER[place - 1]).start()
    make(0)
    give(EXCHANGE_ORDER[-1]).start()
    keep = pltpu.make_async_copy(made_ref.at[0], out_ref.at[mine], own_sem.at[1])
    keep.start()
    all_sent(0)
    all_sent(1)
    keep.wait()
    for step in EXCHANGE_ORDER:
        give(step).wait()


def shards(queries, key_heads, value_tensor, distance_use, block_pick):
    heads, tokens, width = queries.shape
    blocks = tokens // BLOCK
    head_devices = lax.axis_size("head")
    vmem = pl.BlockSpec(memory_space=pltpu.VMEM)
    smem = pl.BlockSpec(memory_space=pltpu.SMEM)
    anywhere = pl.BlockSpec(memory_space=pl.ANY)
    return pl.pallas_call(
        kernel,
        out_shape=jax.ShapeDtypeStruct((heads * head_devices, tokens // head_devices, width), queries.dtype),
        in_specs=[anywhere, vmem, vmem, smem, smem],
        out_specs=anywhere,
        scratch_shapes=[
            pltpu.VMEM((heads, tokens, width), jnp.bfloat16),
            pltpu.VMEM((LEVELS, blocks, BLOCK, width), jnp.bfloat16),
            pltpu.VMEM((LEVELS, blocks, BLOCK, width), jnp.bfloat16),
            pltpu.VMEM((2, blocks - FORWARD_BLOCKS, BLOCK, width), jnp.bfloat16),
            pltpu.VMEM((blocks, heads * BLOCK, width), jnp.float32),
            pltpu.VMEM((blocks, heads * BLOCK, width), jnp.float32),
            pltpu.VMEM((blocks, heads * BLOCK, LEVELS * BLOCK), jnp.bfloat16),
            pltpu.VMEM((blocks, heads, BLOCK, width), jnp.bfloat16),
            pltpu.SemaphoreType.DMA((2, 7)),
            pltpu.SemaphoreType.DMA((2, 7)),
            pltpu.SemaphoreType.DMA((8,)),
            pltpu.SemaphoreType.DMA((8,)),
            pltpu.SemaphoreType.DMA((2,)),
        ],
        compiler_params=pltpu.CompilerParams(
            collective_id=0, has_side_effects=True, vmem_limit_bytes=60 * 1024 * 1024
        ),
        name="power_attention",
    )(
        queries,
        key_heads.reshape(1, blocks, BLOCK, width),
        value_tensor.reshape(1, blocks, BLOCK, width),
        distance_use,
        block_pick,
    )


def solution(mesh):
    placed = (
        P("head", "ctx", None),
        P("head", "ctx", None),
        P("head", "ctx", None),
        P("ctx", None),
        P("ctx", None),
    )
    return jax.shard_map(
        shards,
        mesh=mesh,
        in_specs=placed,
        out_specs=P(None, ("ctx", "head"), None),
        check_vma=False,
    )
```

```python
import functools
import math

import jax
import jax.numpy as jnp
from jax import lax
from jax.experimental import pallas as pl
from jax.experimental.pallas import tpu as pltpu
from jax.sharding import PartitionSpec as P

BLOCK = 128
LEVELS = 5
Y_COUNT = 4
FORWARD_BLOCKS = 3
Y1, Y2, Z1, Z2, Z4F, RELAY, Z4B, Y_RELAY, Y2_BACK = range(9)
X_COUNT = 4
DIRECT, SIBLING, LEG1, LEG2 = 0, 4, 5, 9


def kernel(
    q_hbm, k_ref, v_ref, use_ref, pick_ref, out_ref,
    q_ref, far_keys, far_values, relay_ref, y_relay_ref, total_ref, inverse_ref, weight_ref, made_ref, passing_ref,
    send_sem, recv_sem, out_send_sem, out_recv_sem, own_sem,
):
    heads, tokens, width = q_ref.shape
    blocks = tokens // BLOCK
    ctx = lax.axis_index("ctx")
    head = lax.axis_index("head")
    shards = lax.axis_size("ctx")
    head_devices = lax.axis_size("head")
    z = ctx // Y_COUNT
    y = ctx % Y_COUNT
    along_z = lambda steps: lax.rem(ctx + (steps * Y_COUNT) % shards, shards)
    along_y = lambda steps: z * Y_COUNT + lax.rem(y + steps % Y_COUNT, Y_COUNT)

    take_queries = pltpu.make_async_copy(q_hbm, q_ref, own_sem.at[0])
    take_queries.start()

    barrier = pltpu.get_barrier_semaphore()
    ctx_peers = [along_z(s) for s in (1, -1, 2, -2, 3, -3)] + [along_y(s) for s in (1, -1)]
    for peer in ctx_peers:
        pl.semaphore_signal(barrier, inc=1, device_id={"ctx": peer}, device_id_type=pl.DeviceIdType.MESH)
    for step in range(1, head_devices):
        pl.semaphore_signal(
            barrier, inc=1, device_id={"head": lax.rem(head + step, head_devices)},
            device_id_type=pl.DeviceIdType.MESH,
        )
    pl.semaphore_wait(barrier, len(ctx_peers) + head_devices - 1)

    own = (k_ref.at[0], v_ref.at[0])
    far = (far_keys, far_values)
    top = pl.ds(0, FORWARD_BLOCKS)
    rest = pl.ds(FORWARD_BLOCKS, blocks - FORWARD_BLOCKS)

    def copy(kind, lane, source, target, peer):
        return pltpu.make_async_remote_copy(
            src_ref=source, dst_ref=target,
            send_sem=send_sem.at[kind, lane], recv_sem=recv_sem.at[kind, lane],
            device_id={"ctx": peer}, device_id_type=pl.DeviceIdType.MESH,
        )

    def near_y1(t): return copy(t, Y1, own[t], far[t].at[0], along_y(1))
    def wrap_y1(t): return copy(t, Y1, far[t].at[2], far[t].at[0], along_y(1))
    def forward_y2(t): return copy(t, Y2, far[t].at[0], far[t].at[1], along_y(1))
    def hop_y_relay(t): return copy(t, Y_RELAY, far[t].at[2], y_relay_ref.at[t], along_y(-1))
    def back_y2(t): return copy(t, Y2_BACK, y_relay_ref.at[t], far[t].at[1], along_y(-1))
    def hop_z1(t): return copy(t, Z1, own[t], far[t].at[2], along_z(1))
    def hop_z2(t): return copy(t, Z2, far[t].at[2], far[t].at[3], along_z(1))
    def hop_z4f(t): return copy(t, Z4F, far[t].at[3, top], far[t].at[4, top], along_z(2))
    def hop_relay(t): return copy(t, RELAY, own[t].at[rest], relay_ref.at[t], along_z(-3))
    def hop_z4b(t): return copy(t, Z4B, relay_ref.at[t], far[t].at[4, rest], along_z(-1))

    relays = (z >= 5) | (z == 0)
    forwards = (z >= 2) & (z <= 5)

    def first(t):
        pl.when(z < 7)(lambda: hop_z1(t).start())
        pl.when(z < 4)(lambda: hop_relay(t).start())
        pl.when(y < 3)(lambda: near_y1(t).start())

    def second(t):
        @pl.when(z >= 1)
        def _():
            hop_z1(t).wait_recv()
            pl.when(z <= 6)(lambda: hop_z2(t).start())
            pl.when(y == 3)(lambda: wrap_y1(t).start())
            pl.when(y == 2)(lambda: hop_y_relay(t).start())

        @pl.when((y == 1) | (y == 2))
        def _():
            near_y1(t).wait_recv()
            forward_y2(t).start()

    def third(t):
        pl.when(z >= 2)(lambda: hop_z2(t).wait_recv())
        pl.when(forwards)(lambda: hop_z4f(t).start())

    def fourth(t):
        @pl.when((y == 0) & (z >= 1))
        def _():
            near_y1(t).wait_recv()
            forward_y2(t).start()

        @pl.when((y == 1) & (z >= 1))
        def _():
            hop_y_relay(t).wait_recv()
            back_y2(t).start()

        @pl.when(relays)
        def _():
            hop_relay(t).wait_recv()
            hop_z4b(t).start()

    def last(t):
        pl.when(y == 3)(lambda: near_y1(t).wait_recv())
        pl.when((y >= 2) | ((y == 1) & (z >= 1)))(lambda: forward_y2(t).wait_recv())
        pl.when((y == 0) & (z >= 1))(lambda: back_y2(t).wait_recv())

        @pl.when(z >= 4)
        def _():
            hop_z4f(t).wait_recv()
            hop_z4b(t).wait_recv()

    def all_sent(t):
        pl.when(z < 7)(lambda: hop_z1(t).wait_send())
        pl.when(z < 4)(lambda: hop_relay(t).wait_send())
        pl.when((y < 3) | (z >= 1))(lambda: near_y1(t).wait_send())
        pl.when((y == 1) | (y == 2) | ((y == 0) & (z >= 1)))(lambda: forward_y2(t).wait_send())
        pl.when((y == 2) & (z >= 1))(lambda: hop_y_relay(t).wait_send())
        pl.when((y == 1) & (z >= 1))(lambda: back_y2(t).wait_send())
        pl.when((z >= 1) & (z <= 6))(lambda: hop_z2(t).wait_send())
        pl.when(forwards)(lambda: hop_z4f(t).wait_send())
        pl.when(relays)(lambda: hop_z4b(t).wait_send())

    first(0)
    for level in range(LEVELS):
        @pl.when(ctx < 2**level)
        def _(level=level):
            nothing = jnp.zeros((blocks, BLOCK, width), far_keys.dtype)
            far_keys[level] = nothing
            far_values[level] = nothing

    take_queries.wait()
    second(0)
    third(0)
    fourth(0)
    first(1)
    last(0)

    def picked(t, block):
        return jnp.concatenate(
            [far[t][level, pick_ref[block, level]] for level in range(LEVELS)], axis=0
        )

    exponent_scale = math.log2(math.e) / math.sqrt(width)
    bias = []
    for level in range(LEVELS):
        live = use_ref[0, level] * jnp.where(ctx >= 2**level, 1, 0)
        bias.append(jnp.full((1, BLOCK), (live.astype(jnp.float32) - 1.0) * 3e38, jnp.float32))
    bias = jnp.concatenate(bias, axis=1)
    rows = 2 * BLOCK

    def score_group(group):
        before = group * 2 * BLOCK
        near_width = before + 2 * BLOCK

        def body(step, carry):
            in_group = step // 4
            block = group * 2 + in_group
            pair = step % 4
            first_row = pl.multiple_of(block * BLOCK, BLOCK)
            row_slice = pl.ds(pl.multiple_of(pair * rows, rows), rows)
            q_now = q_ref[pl.ds(pair * 2, 2), pl.ds(first_row, BLOCK), :].reshape(rows, width)
            keys = jnp.concatenate([k_ref[0, : near_width // BLOCK].reshape(near_width, width), picked(0, block)], axis=0)
            scores = lax.dot_general(
                q_now, keys, (((1,), (1,)), ((), ())), preferred_element_type=jnp.float32
            )
            row_pos = lax.broadcasted_iota(jnp.int32, (rows, rows), 0) % BLOCK + in_group * BLOCK
            col_pos = lax.broadcasted_iota(jnp.int32, (rows, rows), 1)
            diagonal = jnp.where(col_pos <= row_pos, scores[:, before:near_width], -jnp.inf)
            distant = scores[:, near_width:] + bias
            parts = [scores[:, :before]] if group else []
            scores = jnp.concatenate(parts + [diagonal, distant], axis=1)
            peak = jnp.max(scores, axis=1, keepdims=True)
            weights = jnp.exp2((scores - peak) * exponent_scale)
            row_total = jnp.sum(weights, axis=1, keepdims=True)
            rounded = weights.astype(jnp.bfloat16)
            weight_ref[block, row_slice, :] = rounded[:, near_width:]
            total_ref[block, row_slice, :] = jnp.dot(
                rounded[:, :near_width], v_ref[0, : near_width // BLOCK].reshape(near_width, width), preferred_element_type=jnp.float32
            )
            inverse_ref[block, row_slice, :] = jnp.broadcast_to(1.0 / row_total, (rows, width))
            return carry

        lax.fori_loop(0, 8, body, 0)

    score_group(0)
    second(1)
    score_group(1)
    score_group(2)
    third(1)
    fourth(1)
    score_group(3)
    last(1)

    x = head // 2
    core = head % 2
    half = heads // 2

    def device(x_steps, to_core):
        return lax.rem(x + x_steps, X_COUNT) * 2 + to_core

    targets = [device(2, 0), device(2, 1), device(1, 0), device(3, 0), device(1, 1), device(3, 1), device(0, 1 - core), head]

    def make(slot):
        block = targets[slot]
        values = picked(1, block)

        def body(pair, carry):
            row_slice = pl.ds(pl.multiple_of(pair * rows, rows), rows)
            distant = jnp.dot(weight_ref[block, row_slice, :], values, preferred_element_type=jnp.float32)
            result = (total_ref[block, row_slice, :] + distant) * inverse_ref[block, row_slice, :]
            made_ref[slot, pl.ds(pair * 2, 2)] = result.astype(made_ref.dtype).reshape(2, BLOCK, width)
            return carry

        lax.fori_loop(0, heads // 2, body, 0)

    def give(source, target, sent, received, to_head):
        return pltpu.make_async_remote_copy(
            src_ref=source, dst_ref=target,
            send_sem=out_send_sem.at[sent], recv_sem=out_recv_sem.at[received],
            device_id={"head": to_head}, device_id_type=pl.DeviceIdType.MESH,
        )

    mine = pl.ds(head * heads, heads)

    def leg1(part, to_core):
        source = made_ref.at[to_core, pl.ds(part * half, half)]
        place = LEG1 + part * 2 + to_core
        return give(source, passing_ref.at[part, to_core], place, place, device((1, 3)[part], core))

    def leg2(part, to_core, received):
        source_head = device((3, 1)[part], core)
        target = out_ref.at[pl.ds(source_head * heads + part * half, half)]
        return give(
            passing_ref.at[part, to_core], target, LEG2 + part * 2 + to_core, received,
            device((1, 3)[part], to_core),
        )

    def direct(slot, received):
        return give(made_ref.at[slot], out_ref.at[mine], DIRECT + slot - 2, received, targets[slot])

    def start(slot):
        if slot < 2:
            leg1(0, slot).start()
            leg1(1, slot).start()
        elif slot < 6:
            direct(slot, DIRECT + (slot % 2) * 2 + core).start()
        else:
            direct(slot, SIBLING).start()

    for slot in range(8):
        make(slot)
        if slot:
            start(slot - 1)
    keep = pltpu.make_async_copy(made_ref.at[7], out_ref.at[mine], own_sem.at[1])
    keep.start()
    for part in range(2):
        for to_core in range(2):
            leg1(part, to_core).wait_recv()
            leg2(part, to_core, LEG2 + part * 2 + core).start()
    all_sent(0)
    all_sent(1)
    keep.wait()
    for slot in range(2, 7):
        direct(slot, DIRECT + slot - 2).wait()
    for part in range(2):
        for to_core in range(2):
            leg1(part, to_core).wait_send()
            leg2(part, to_core, LEG2 + part * 2 + to_core).wait()


def shards(queries, key_heads, value_tensor, distance_use, block_pick):
    heads, tokens, width = queries.shape
    blocks = tokens // BLOCK
    head_devices = lax.axis_size("head")
    vmem = pl.BlockSpec(memory_space=pltpu.VMEM)
    smem = pl.BlockSpec(memory_space=pltpu.SMEM)
    anywhere = pl.BlockSpec(memory_space=pl.ANY)
    return pl.pallas_call(
        kernel,
        out_shape=jax.ShapeDtypeStruct((heads * head_devices, tokens // head_devices, width), queries.dtype),
        in_specs=[anywhere, vmem, vmem, smem, smem],
        out_specs=anywhere,
        scratch_shapes=[
            pltpu.VMEM((heads, tokens, width), jnp.bfloat16),
            pltpu.VMEM((LEVELS, blocks, BLOCK, width), jnp.bfloat16),
            pltpu.VMEM((LEVELS, blocks, BLOCK, width), jnp.bfloat16),
            pltpu.VMEM((2, blocks - FORWARD_BLOCKS, BLOCK, width), jnp.bfloat16),
            pltpu.VMEM((2, blocks, BLOCK, width), jnp.bfloat16),
            pltpu.VMEM((blocks, heads * BLOCK, width), jnp.float32),
            pltpu.VMEM((blocks, heads * BLOCK, width), jnp.float32),
            pltpu.VMEM((blocks, heads * BLOCK, LEVELS * BLOCK), jnp.bfloat16),
            pltpu.VMEM((blocks, heads, BLOCK, width), jnp.bfloat16),
            pltpu.VMEM((2, 2, heads // 2, BLOCK, width), jnp.bfloat16),
            pltpu.SemaphoreType.DMA((2, 9)),
            pltpu.SemaphoreType.DMA((2, 9)),
            pltpu.SemaphoreType.DMA((13,)),
            pltpu.SemaphoreType.DMA((13,)),
            pltpu.SemaphoreType.DMA((2,)),
        ],
        compiler_params=pltpu.CompilerParams(
            collective_id=0, has_side_effects=True, vmem_limit_bytes=60 * 1024 * 1024
        ),
        name="power_attention",
    )(
        queries,
        key_heads.reshape(1, blocks, BLOCK, width),
        value_tensor.reshape(1, blocks, BLOCK, width),
        distance_use,
        block_pick,
    )


def solution(mesh):
    placed = (
        P("head", "ctx", None),
        P("head", "ctx", None),
        P("head", "ctx", None),
        P("ctx", None),
        P("ctx", None),
    )
    return jax.shard_map(
        shards,
        mesh=mesh,
        in_specs=placed,
        out_specs=P(None, ("ctx", "head"), None),
        check_vma=False,
    )
```

```python
import functools
import math

import jax
import jax.numpy as jnp
from jax import lax
from jax.experimental import pallas as pl
from jax.experimental.pallas import tpu as pltpu
from jax.sharding import PartitionSpec as P

BLOCK = 128
LEVELS = 5
Y_COUNT = 4
FORWARD_BLOCKS = 3
Y1, Y2, Z1, Z2, Z4F, RELAY, Z4B, Y_RELAY, Y2_BACK = range(9)
X_COUNT = 4
STEP_HEADS = 2
UNROLL = 1
DIRECT, SIBLING, LEG1, LEG2 = 0, 4, 5, 9


def kernel(
    q_hbm, k_ref, v_ref, use_ref, pick_ref, out_ref,
    q_ref, far_keys, far_values, relay_ref, y_relay_ref, total_ref, inverse_ref, weight_ref, made_ref, passing_ref,
    near_0, near_1, near_2, near_3,
    send_sem, recv_sem, out_send_sem, out_recv_sem, own_sem,
):
    heads, tokens, width = q_ref.shape
    blocks = tokens // BLOCK
    ctx = lax.axis_index("ctx")
    head = lax.axis_index("head")
    shards = lax.axis_size("ctx")
    head_devices = lax.axis_size("head")
    z = ctx // Y_COUNT
    y = ctx % Y_COUNT
    along_z = lambda steps: lax.rem(ctx + (steps * Y_COUNT) % shards, shards)
    along_y = lambda steps: z * Y_COUNT + lax.rem(y + steps % Y_COUNT, Y_COUNT)

    take_queries = pltpu.make_async_copy(q_hbm, q_ref, own_sem.at[0])
    take_queries.start()

    barrier = pltpu.get_barrier_semaphore()
    ctx_peers = [along_z(s) for s in (1, -1, 2, -2, 3, -3)] + [along_y(s) for s in (1, -1)]
    for peer in ctx_peers:
        pl.semaphore_signal(barrier, inc=1, device_id={"ctx": peer}, device_id_type=pl.DeviceIdType.MESH)
    for step in range(1, head_devices):
        pl.semaphore_signal(
            barrier, inc=1, device_id={"head": lax.rem(head + step, head_devices)},
            device_id_type=pl.DeviceIdType.MESH,
        )
    pl.semaphore_wait(barrier, len(ctx_peers) + head_devices - 1)

    own = (k_ref.at[0], v_ref.at[0])
    far = (far_keys, far_values)
    near_refs = (near_0, near_1, near_2, near_3)
    top = pl.ds(0, FORWARD_BLOCKS)
    rest = pl.ds(FORWARD_BLOCKS, blocks - FORWARD_BLOCKS)

    def copy(kind, lane, source, target, peer):
        return pltpu.make_async_remote_copy(
            src_ref=source, dst_ref=target,
            send_sem=send_sem.at[kind, lane], recv_sem=recv_sem.at[kind, lane],
            device_id={"ctx": peer}, device_id_type=pl.DeviceIdType.MESH,
        )

    def near_y1(t): return copy(t, Y1, own[t], far[t].at[0], along_y(1))
    def wrap_y1(t): return copy(t, Y1, far[t].at[2], far[t].at[0], along_y(1))
    def forward_y2(t): return copy(t, Y2, far[t].at[0], far[t].at[1], along_y(1))
    def hop_y_relay(t): return copy(t, Y_RELAY, far[t].at[2], y_relay_ref.at[t], along_y(-1))
    def back_y2(t): return copy(t, Y2_BACK, y_relay_ref.at[t], far[t].at[1], along_y(-1))
    def hop_z1(t): return copy(t, Z1, own[t], far[t].at[2], along_z(1))
    def hop_z2(t): return copy(t, Z2, far[t].at[2], far[t].at[3], along_z(1))
    def hop_z4f(t): return copy(t, Z4F, far[t].at[3, top], far[t].at[4, top], along_z(2))
    def hop_relay(t): return copy(t, RELAY, own[t].at[rest], relay_ref.at[t], along_z(-3))
    def hop_z4b(t): return copy(t, Z4B, relay_ref.at[t], far[t].at[4, rest], along_z(-1))

    relays = (z >= 5) | (z == 0)
    forwards = (z >= 2) & (z <= 5)

    def first(t):
        pl.when(z < 7)(lambda: hop_z1(t).start())
        pl.when(z < 4)(lambda: hop_relay(t).start())
        pl.when(y < 3)(lambda: near_y1(t).start())

    def second(t):
        @pl.when(z >= 1)
        def _():
            hop_z1(t).wait_recv()
            pl.when(z <= 6)(lambda: hop_z2(t).start())
            pl.when(y == 3)(lambda: wrap_y1(t).start())
            pl.when(y == 2)(lambda: hop_y_relay(t).start())

        @pl.when((y == 1) | (y == 2))
        def _():
            near_y1(t).wait_recv()
            forward_y2(t).start()

    def third(t):
        pl.when(z >= 2)(lambda: hop_z2(t).wait_recv())
        pl.when(forwards)(lambda: hop_z4f(t).start())

    def fourth(t):
        @pl.when((y == 0) & (z >= 1))
        def _():
            near_y1(t).wait_recv()
            forward_y2(t).start()

        @pl.when((y == 1) & (z >= 1))
        def _():
            hop_y_relay(t).wait_recv()
            back_y2(t).start()

        @pl.when(relays)
        def _():
            hop_relay(t).wait_recv()
            hop_z4b(t).start()

    def last(t):
        pl.when(y == 3)(lambda: near_y1(t).wait_recv())
        pl.when((y >= 2) | ((y == 1) & (z >= 1)))(lambda: forward_y2(t).wait_recv())
        pl.when((y == 0) & (z >= 1))(lambda: back_y2(t).wait_recv())

        @pl.when(z >= 4)
        def _():
            hop_z4f(t).wait_recv()
            hop_z4b(t).wait_recv()

    def all_sent(t):
        pl.when(z < 7)(lambda: hop_z1(t).wait_send())
        pl.when(z < 4)(lambda: hop_relay(t).wait_send())
        pl.when((y < 3) | (z >= 1))(lambda: near_y1(t).wait_send())
        pl.when((y == 1) | (y == 2) | ((y == 0) & (z >= 1)))(lambda: forward_y2(t).wait_send())
        pl.when((y == 2) & (z >= 1))(lambda: hop_y_relay(t).wait_send())
        pl.when((y == 1) & (z >= 1))(lambda: back_y2(t).wait_send())
        pl.when((z >= 1) & (z <= 6))(lambda: hop_z2(t).wait_send())
        pl.when(forwards)(lambda: hop_z4f(t).wait_send())
        pl.when(relays)(lambda: hop_z4b(t).wait_send())

    first(0)
    for level in range(LEVELS):
        @pl.when(ctx < 2**level)
        def _(level=level):
            nothing = jnp.zeros((blocks, BLOCK, width), far_keys.dtype)
            far_keys[level] = nothing
            far_values[level] = nothing

    take_queries.wait()

    def picked(t, block):
        return jnp.concatenate(
            [far[t][level, pick_ref[block, level]] for level in range(LEVELS)], axis=0
        )

    exponent_scale = math.log2(math.e) / math.sqrt(width)
    bias = []
    for level in range(LEVELS):
        live = use_ref[0, level] * jnp.where(ctx >= 2**level, 1, 0)
        bias.append(jnp.full((1, BLOCK), (live.astype(jnp.float32) - 1.0) * 3e38, jnp.float32))
    bias = jnp.concatenate(bias, axis=1)
    rows = 2 * BLOCK
    step_rows = STEP_HEADS * BLOCK
    steps_per_block = heads // STEP_HEADS

    def group_shape(group):
        before = group * 2 * BLOCK
        return before, before + 2 * BLOCK

    def place_of(step, group):
        in_group = step // steps_per_block
        part = step % steps_per_block
        block = group * 2 + in_group
        first_row = pl.multiple_of(block * BLOCK, BLOCK)
        row_slice = pl.ds(pl.multiple_of(part * step_rows, step_rows), step_rows)
        q_now = q_ref[pl.ds(part * STEP_HEADS, STEP_HEADS), pl.ds(first_row, BLOCK), :]
        return in_group, block, row_slice, q_now.reshape(step_rows, width)

    def lane_peak(scores):
        return functools.reduce(
            jnp.maximum, [scores[:, c : c + BLOCK] for c in range(0, scores.shape[1], BLOCK)]
        )

    def score_near(group):
        before, near_width = group_shape(group)

        def body(step, carry):
            in_group, block, row_slice, q_now = place_of(step, group)
            keys = k_ref[0, : near_width // BLOCK].reshape(near_width, width)
            scores = lax.dot_general(
                q_now, keys, (((1,), (1,)), ((), ())), preferred_element_type=jnp.float32
            )
            row_pos = lax.broadcasted_iota(jnp.int32, (step_rows, rows), 0) % BLOCK + in_group * BLOCK
            col_pos = lax.broadcasted_iota(jnp.int32, (step_rows, rows), 1)
            diagonal = jnp.where(col_pos <= row_pos, scores[:, before:], -jnp.inf)
            parts = [scores[:, :before]] if group else []
            scores = jnp.concatenate(parts + [diagonal], axis=1)
            near_refs[group][in_group, row_slice, :] = scores
            inverse_ref[block, row_slice, :] = lane_peak(scores)
            return carry

        lax.fori_loop(0, 2 * steps_per_block, body, 0, unroll=UNROLL)

    def score_far(group):
        _, near_width = group_shape(group)

        def body(step, carry):
            in_group, block, row_slice, q_now = place_of(step, group)
            distant = lax.dot_general(
                q_now, picked(0, block), (((1,), (1,)), ((), ())), preferred_element_type=jnp.float32
            ) + bias
            peak = jnp.max(
                jnp.maximum(inverse_ref[block, row_slice, :], lane_peak(distant)), axis=1, keepdims=True
            )
            near_weights = jnp.exp2((near_refs[group][in_group, row_slice, :] - peak) * exponent_scale)
            far_weights = jnp.exp2((distant - peak) * exponent_scale)
            row_total = jnp.sum(near_weights, axis=1, keepdims=True) + jnp.sum(
                far_weights, axis=1, keepdims=True
            )
            weight_ref[block, row_slice, :] = far_weights.astype(jnp.bfloat16)
            total_ref[block, row_slice, :] = jnp.dot(
                near_weights.astype(jnp.bfloat16),
                v_ref[0, : near_width // BLOCK].reshape(near_width, width),
                preferred_element_type=jnp.float32,
            )
            inverse_ref[block, row_slice, :] = jnp.broadcast_to(1.0 / row_total, (step_rows, width))
            return carry

        lax.fori_loop(0, 2 * steps_per_block, body, 0, unroll=UNROLL)

    score_near(0)
    score_near(1)
    second(0)
    score_near(2)
    score_near(3)
    third(0)
    fourth(0)
    first(1)
    last(0)

    score_far(0)
    second(1)
    score_far(1)
    score_far(2)
    third(1)
    fourth(1)
    score_far(3)
    last(1)

    x = head // 2
    core = head % 2
    half = heads // 2

    def device(x_steps, to_core):
        return lax.rem(x + x_steps, X_COUNT) * 2 + to_core

    targets = [device(2, 0), device(2, 1), device(1, 0), device(3, 0), device(1, 1), device(3, 1), device(0, 1 - core), head]

    def make(slot):
        block = targets[slot]
        values = picked(1, block)

        def body(pair, carry):
            row_slice = pl.ds(pl.multiple_of(pair * rows, rows), rows)
            distant = jnp.dot(weight_ref[block, row_slice, :], values, preferred_element_type=jnp.float32)
            result = (total_ref[block, row_slice, :] + distant) * inverse_ref[block, row_slice, :]
            made_ref[slot, pl.ds(pair * 2, 2)] = result.astype(made_ref.dtype).reshape(2, BLOCK, width)
            return carry

        lax.fori_loop(0, heads // 2, body, 0)

    def give(source, target, sent, received, to_head):
        return pltpu.make_async_remote_copy(
            src_ref=source, dst_ref=target,
            send_sem=out_send_sem.at[sent], recv_sem=out_recv_sem.at[received],
            device_id={"head": to_head}, device_id_type=pl.DeviceIdType.MESH,
        )

    mine = pl.ds(head * heads, heads)

    def leg1(part, to_core):
        source = made_ref.at[to_core, pl.ds(part * half, half)]
        place = LEG1 + part * 2 + to_core
        return give(source, passing_ref.at[part, to_core], place, place, device((1, 3)[part], core))

    def leg2(part, to_core, received):
        source_head = device((3, 1)[part], core)
        target = out_ref.at[pl.ds(source_head * heads + part * half, half)]
        return give(
            passing_ref.at[part, to_core], target, LEG2 + part * 2 + to_core, received,
            device((1, 3)[part], to_core),
        )

    def direct(slot, received):
        return give(made_ref.at[slot], out_ref.at[mine], DIRECT + slot - 2, received, targets[slot])

    def start(slot):
        if slot < 2:
            leg1(0, slot).start()
            leg1(1, slot).start()
        elif slot < 6:
            direct(slot, DIRECT + (slot % 2) * 2 + core).start()
        else:
            direct(slot, SIBLING).start()

    for slot in range(8):
        make(slot)
        if slot:
            start(slot - 1)
    keep = pltpu.make_async_copy(made_ref.at[7], out_ref.at[mine], own_sem.at[1])
    keep.start()
    for part in range(2):
        for to_core in range(2):
            leg1(part, to_core).wait_recv()
            leg2(part, to_core, LEG2 + part * 2 + core).start()
    all_sent(0)
    all_sent(1)
    keep.wait()
    for slot in range(2, 7):
        direct(slot, DIRECT + slot - 2).wait()
    for part in range(2):
        for to_core in range(2):
            leg1(part, to_core).wait_send()
            leg2(part, to_core, LEG2 + part * 2 + to_core).wait()


def shards(queries, key_heads, value_tensor, distance_use, block_pick):
    heads, tokens, width = queries.shape
    blocks = tokens // BLOCK
    head_devices = lax.axis_size("head")
    vmem = pl.BlockSpec(memory_space=pltpu.VMEM)
    smem = pl.BlockSpec(memory_space=pltpu.SMEM)
    anywhere = pl.BlockSpec(memory_space=pl.ANY)
    return pl.pallas_call(
        kernel,
        out_shape=jax.ShapeDtypeStruct((heads * head_devices, tokens // head_devices, width), queries.dtype),
        in_specs=[anywhere, vmem, vmem, smem, smem],
        out_specs=anywhere,
        scratch_shapes=[
            pltpu.VMEM((heads, tokens, width), jnp.bfloat16),
            pltpu.VMEM((LEVELS, blocks, BLOCK, width), jnp.bfloat16),
            pltpu.VMEM((LEVELS, blocks, BLOCK, width), jnp.bfloat16),
            pltpu.VMEM((2, blocks - FORWARD_BLOCKS, BLOCK, width), jnp.bfloat16),
            pltpu.VMEM((2, blocks, BLOCK, width), jnp.bfloat16),
            pltpu.VMEM((blocks, heads * BLOCK, width), jnp.float32),
            pltpu.VMEM((blocks, heads * BLOCK, width), jnp.float32),
            pltpu.VMEM((blocks, heads * BLOCK, LEVELS * BLOCK), jnp.bfloat16),
            pltpu.VMEM((blocks, heads, BLOCK, width), jnp.bfloat16),
            pltpu.VMEM((2, 2, heads // 2, BLOCK, width), jnp.bfloat16),
            *[pltpu.VMEM((2, heads * BLOCK, 2 * BLOCK * (group + 1)), jnp.float32) for group in range(4)],
            pltpu.SemaphoreType.DMA((2, 9)),
            pltpu.SemaphoreType.DMA((2, 9)),
            pltpu.SemaphoreType.DMA((13,)),
            pltpu.SemaphoreType.DMA((13,)),
            pltpu.SemaphoreType.DMA((2,)),
        ],
        compiler_params=pltpu.CompilerParams(
            collective_id=0, has_side_effects=True, vmem_limit_bytes=60 * 1024 * 1024
        ),
        name="power_attention",
    )(
        queries,
        key_heads.reshape(1, blocks, BLOCK, width),
        value_tensor.reshape(1, blocks, BLOCK, width),
        distance_use,
        block_pick,
    )


def solution(mesh):
    placed = (
        P("head", "ctx", None),
        P("head", "ctx", None),
        P("head", "ctx", None),
        P("ctx", None),
        P("ctx", None),
    )
    return jax.shard_map(
        shards,
        mesh=mesh,
        in_specs=placed,
        out_specs=P(None, ("ctx", "head"), None),
        check_vma=False,
    )
```

```python
import functools
import math

import jax
import jax.numpy as jnp
from jax import lax
from jax.experimental import pallas as pl
from jax.experimental.pallas import tpu as pltpu
from jax.sharding import PartitionSpec as P

BLOCK = 128
LEVELS = 5
Y_COUNT = 4
FORWARD_BLOCKS = 3
Y1, Y2, Z1, Z2, Z4F, RELAY, Z4B, Y_RELAY, Y2_BACK = range(9)
X_COUNT = 4
STEP_HEADS = 2
UNROLL = 2
DIRECT, SIBLING, LEG1, LEG2 = 0, 4, 5, 9


def kernel(
    q_hbm, k_ref, v_ref, use_ref, pick_ref, out_ref,
    q_ref, far_keys, far_values, relay_ref, y_relay_ref, total_ref, inverse_ref, weight_ref, made_ref, passing_ref,
    near_0, near_1, near_2, near_3,
    send_sem, recv_sem, out_send_sem, out_recv_sem, own_sem,
):
    heads, tokens, width = q_ref.shape
    blocks = tokens // BLOCK
    ctx = lax.axis_index("ctx")
    head = lax.axis_index("head")
    shards = lax.axis_size("ctx")
    head_devices = lax.axis_size("head")
    z = ctx // Y_COUNT
    y = ctx % Y_COUNT
    along_z = lambda steps: lax.rem(ctx + (steps * Y_COUNT) % shards, shards)
    along_y = lambda steps: z * Y_COUNT + lax.rem(y + steps % Y_COUNT, Y_COUNT)

    take_queries = pltpu.make_async_copy(q_hbm, q_ref, own_sem.at[0])
    take_queries.start()

    barrier = pltpu.get_barrier_semaphore()
    ctx_peers = [along_z(s) for s in (1, -1, 2, -2, 3, -3)] + [along_y(s) for s in (1, -1)]
    for peer in ctx_peers:
        pl.semaphore_signal(barrier, inc=1, device_id={"ctx": peer}, device_id_type=pl.DeviceIdType.MESH)
    for step in range(1, head_devices):
        pl.semaphore_signal(
            barrier, inc=1, device_id={"head": lax.rem(head + step, head_devices)},
            device_id_type=pl.DeviceIdType.MESH,
        )
    pl.semaphore_wait(barrier, len(ctx_peers) + head_devices - 1)

    own = (k_ref.at[0], v_ref.at[0])
    far = (far_keys, far_values)
    near_refs = (near_0, near_1, near_2, near_3)
    top = pl.ds(0, FORWARD_BLOCKS)
    rest = pl.ds(FORWARD_BLOCKS, blocks - FORWARD_BLOCKS)

    def copy(kind, lane, source, target, peer):
        return pltpu.make_async_remote_copy(
            src_ref=source, dst_ref=target,
            send_sem=send_sem.at[kind, lane], recv_sem=recv_sem.at[kind, lane],
            device_id={"ctx": peer}, device_id_type=pl.DeviceIdType.MESH,
        )

    def near_y1(t): return copy(t, Y1, own[t], far[t].at[0], along_y(1))
    def wrap_y1(t): return copy(t, Y1, far[t].at[2], far[t].at[0], along_y(1))
    def forward_y2(t): return copy(t, Y2, far[t].at[0], far[t].at[1], along_y(1))
    def hop_y_relay(t): return copy(t, Y_RELAY, far[t].at[2], y_relay_ref.at[t], along_y(-1))
    def back_y2(t): return copy(t, Y2_BACK, y_relay_ref.at[t], far[t].at[1], along_y(-1))
    def hop_z1(t): return copy(t, Z1, own[t], far[t].at[2], along_z(1))
    def hop_z2(t): return copy(t, Z2, far[t].at[2], far[t].at[3], along_z(1))
    def hop_z4f(t): return copy(t, Z4F, far[t].at[3, top], far[t].at[4, top], along_z(2))
    def hop_relay(t): return copy(t, RELAY, own[t].at[rest], relay_ref.at[t], along_z(-3))
    def hop_z4b(t): return copy(t, Z4B, relay_ref.at[t], far[t].at[4, rest], along_z(-1))

    relays = (z >= 5) | (z == 0)
    forwards = (z >= 2) & (z <= 5)

    def first(t):
        pl.when(z < 7)(lambda: hop_z1(t).start())
        pl.when(z < 4)(lambda: hop_relay(t).start())
        pl.when(y < 3)(lambda: near_y1(t).start())

    def second(t):
        @pl.when(z >= 1)
        def _():
            hop_z1(t).wait_recv()
            pl.when(z <= 6)(lambda: hop_z2(t).start())
            pl.when(y == 3)(lambda: wrap_y1(t).start())
            pl.when(y == 2)(lambda: hop_y_relay(t).start())

        @pl.when((y == 1) | (y == 2))
        def _():
            near_y1(t).wait_recv()
            forward_y2(t).start()

    def third(t):
        pl.when(z >= 2)(lambda: hop_z2(t).wait_recv())
        pl.when(forwards)(lambda: hop_z4f(t).start())

    def fourth(t):
        @pl.when((y == 0) & (z >= 1))
        def _():
            near_y1(t).wait_recv()
            forward_y2(t).start()

        @pl.when((y == 1) & (z >= 1))
        def _():
            hop_y_relay(t).wait_recv()
            back_y2(t).start()

        @pl.when(relays)
        def _():
            hop_relay(t).wait_recv()
            hop_z4b(t).start()

    def last(t):
        pl.when(y == 3)(lambda: near_y1(t).wait_recv())
        pl.when((y >= 2) | ((y == 1) & (z >= 1)))(lambda: forward_y2(t).wait_recv())
        pl.when((y == 0) & (z >= 1))(lambda: back_y2(t).wait_recv())

        @pl.when(z >= 4)
        def _():
            hop_z4f(t).wait_recv()
            hop_z4b(t).wait_recv()

    def all_sent(t):
        pl.when(z < 7)(lambda: hop_z1(t).wait_send())
        pl.when(z < 4)(lambda: hop_relay(t).wait_send())
        pl.when((y < 3) | (z >= 1))(lambda: near_y1(t).wait_send())
        pl.when((y == 1) | (y == 2) | ((y == 0) & (z >= 1)))(lambda: forward_y2(t).wait_send())
        pl.when((y == 2) & (z >= 1))(lambda: hop_y_relay(t).wait_send())
        pl.when((y == 1) & (z >= 1))(lambda: back_y2(t).wait_send())
        pl.when((z >= 1) & (z <= 6))(lambda: hop_z2(t).wait_send())
        pl.when(forwards)(lambda: hop_z4f(t).wait_send())
        pl.when(relays)(lambda: hop_z4b(t).wait_send())

    first(0)
    for level in range(LEVELS):
        @pl.when(ctx < 2**level)
        def _(level=level):
            nothing = jnp.zeros((blocks, BLOCK, width), far_keys.dtype)
            far_keys[level] = nothing
            far_values[level] = nothing

    take_queries.wait()

    def picked(t, block):
        return jnp.concatenate(
            [far[t][level, pick_ref[block, level]] for level in range(LEVELS)], axis=0
        )

    exponent_scale = math.log2(math.e) / math.sqrt(width)
    bias = []
    for level in range(LEVELS):
        live = use_ref[0, level] * jnp.where(ctx >= 2**level, 1, 0)
        bias.append(jnp.full((1, BLOCK), (live.astype(jnp.float32) - 1.0) * 3e38, jnp.float32))
    bias = jnp.concatenate(bias, axis=1)
    rows = 2 * BLOCK
    step_rows = STEP_HEADS * BLOCK
    steps_per_block = heads // STEP_HEADS

    def group_shape(group):
        before = group * 2 * BLOCK
        return before, before + 2 * BLOCK

    def place_of(step, group):
        in_group = step // steps_per_block
        part = step % steps_per_block
        block = group * 2 + in_group
        first_row = pl.multiple_of(block * BLOCK, BLOCK)
        row_slice = pl.ds(pl.multiple_of(part * step_rows, step_rows), step_rows)
        q_now = q_ref[pl.ds(part * STEP_HEADS, STEP_HEADS), pl.ds(first_row, BLOCK), :]
        return in_group, block, row_slice, q_now.reshape(step_rows, width)

    def lane_peak(scores):
        return functools.reduce(
            jnp.maximum, [scores[:, c : c + BLOCK] for c in range(0, scores.shape[1], BLOCK)]
        )

    def score_near(group):
        before, near_width = group_shape(group)

        def body(step, carry):
            in_group, block, row_slice, q_now = place_of(step, group)
            keys = k_ref[0, : near_width // BLOCK].reshape(near_width, width)
            scores = lax.dot_general(
                q_now, keys, (((1,), (1,)), ((), ())), preferred_element_type=jnp.float32
            )
            row_pos = lax.broadcasted_iota(jnp.int32, (step_rows, rows), 0) % BLOCK + in_group * BLOCK
            col_pos = lax.broadcasted_iota(jnp.int32, (step_rows, rows), 1)
            diagonal = jnp.where(col_pos <= row_pos, scores[:, before:], -jnp.inf)
            parts = [scores[:, :before]] if group else []
            scores = jnp.concatenate(parts + [diagonal], axis=1)
            near_refs[group][in_group, row_slice, :] = scores
            inverse_ref[block, row_slice, :] = lane_peak(scores)
            return carry

        lax.fori_loop(0, 2 * steps_per_block, body, 0, unroll=UNROLL)

    def score_far(group):
        _, near_width = group_shape(group)

        def body(step, carry):
            in_group, block, row_slice, q_now = place_of(step, group)
            distant = lax.dot_general(
                q_now, picked(0, block), (((1,), (1,)), ((), ())), preferred_element_type=jnp.float32
            ) + bias
            peak = jnp.max(
                jnp.maximum(inverse_ref[block, row_slice, :], lane_peak(distant)), axis=1, keepdims=True
            )
            near_weights = jnp.exp2((near_refs[group][in_group, row_slice, :] - peak) * exponent_scale)
            far_weights = jnp.exp2((distant - peak) * exponent_scale)
            row_total = jnp.sum(near_weights, axis=1, keepdims=True) + jnp.sum(
                far_weights, axis=1, keepdims=True
            )
            weight_ref[block, row_slice, :] = far_weights.astype(jnp.bfloat16)
            total_ref[block, row_slice, :] = jnp.dot(
                near_weights.astype(jnp.bfloat16),
                v_ref[0, : near_width // BLOCK].reshape(near_width, width),
                preferred_element_type=jnp.float32,
            )
            inverse_ref[block, row_slice, :] = jnp.broadcast_to(1.0 / row_total, (step_rows, width))
            return carry

        lax.fori_loop(0, 2 * steps_per_block, body, 0, unroll=UNROLL)

    score_near(0)
    score_near(1)
    second(0)
    score_near(2)
    score_near(3)
    third(0)
    fourth(0)
    first(1)
    last(0)

    score_far(0)
    second(1)
    score_far(1)
    score_far(2)
    third(1)
    fourth(1)
    score_far(3)
    last(1)

    x = head // 2
    core = head % 2
    half = heads // 2

    def device(x_steps, to_core):
        return lax.rem(x + x_steps, X_COUNT) * 2 + to_core

    targets = [device(2, 0), device(2, 1), device(1, 0), device(3, 0), device(1, 1), device(3, 1), device(0, 1 - core), head]

    def make(slot):
        block = targets[slot]
        values = picked(1, block)

        def body(pair, carry):
            row_slice = pl.ds(pl.multiple_of(pair * rows, rows), rows)
            distant = jnp.dot(weight_ref[block, row_slice, :], values, preferred_element_type=jnp.float32)
            result = (total_ref[block, row_slice, :] + distant) * inverse_ref[block, row_slice, :]
            made_ref[slot, pl.ds(pair * 2, 2)] = result.astype(made_ref.dtype).reshape(2, BLOCK, width)
            return carry

        lax.fori_loop(0, heads // 2, body, 0)

    def give(source, target, sent, received, to_head):
        return pltpu.make_async_remote_copy(
            src_ref=source, dst_ref=target,
            send_sem=out_send_sem.at[sent], recv_sem=out_recv_sem.at[received],
            device_id={"head": to_head}, device_id_type=pl.DeviceIdType.MESH,
        )

    mine = pl.ds(head * heads, heads)

    def leg1(part, to_core):
        source = made_ref.at[to_core, pl.ds(part * half, half)]
        place = LEG1 + part * 2 + to_core
        return give(source, passing_ref.at[part, to_core], place, place, device((1, 3)[part], core))

    def leg2(part, to_core, received):
        source_head = device((3, 1)[part], core)
        target = out_ref.at[pl.ds(source_head * heads + part * half, half)]
        return give(
            passing_ref.at[part, to_core], target, LEG2 + part * 2 + to_core, received,
            device((1, 3)[part], to_core),
        )

    def direct(slot, received):
        return give(made_ref.at[slot], out_ref.at[mine], DIRECT + slot - 2, received, targets[slot])

    def start(slot):
        if slot < 2:
            leg1(0, slot).start()
            leg1(1, slot).start()
        elif slot < 6:
            direct(slot, DIRECT + (slot % 2) * 2 + core).start()
        else:
            direct(slot, SIBLING).start()

    for slot in range(8):
        make(slot)
        if slot:
            start(slot - 1)
    keep = pltpu.make_async_copy(made_ref.at[7], out_ref.at[mine], own_sem.at[1])
    keep.start()
    for part in range(2):
        for to_core in range(2):
            leg1(part, to_core).wait_recv()
            leg2(part, to_core, LEG2 + part * 2 + core).start()
    all_sent(0)
    all_sent(1)
    keep.wait()
    for slot in range(2, 7):
        direct(slot, DIRECT + slot - 2).wait()
    for part in range(2):
        for to_core in range(2):
            leg1(part, to_core).wait_send()
            leg2(part, to_core, LEG2 + part * 2 + to_core).wait()


def shards(queries, key_heads, value_tensor, distance_use, block_pick):
    heads, tokens, width = queries.shape
    blocks = tokens // BLOCK
    head_devices = lax.axis_size("head")
    vmem = pl.BlockSpec(memory_space=pltpu.VMEM)
    smem = pl.BlockSpec(memory_space=pltpu.SMEM)
    anywhere = pl.BlockSpec(memory_space=pl.ANY)
    return pl.pallas_call(
        kernel,
        out_shape=jax.ShapeDtypeStruct((heads * head_devices, tokens // head_devices, width), queries.dtype),
        in_specs=[anywhere, vmem, vmem, smem, smem],
        out_specs=anywhere,
        scratch_shapes=[
            pltpu.VMEM((heads, tokens, width), jnp.bfloat16),
            pltpu.VMEM((LEVELS, blocks, BLOCK, width), jnp.bfloat16),
            pltpu.VMEM((LEVELS, blocks, BLOCK, width), jnp.bfloat16),
            pltpu.VMEM((2, blocks - FORWARD_BLOCKS, BLOCK, width), jnp.bfloat16),
            pltpu.VMEM((2, blocks, BLOCK, width), jnp.bfloat16),
            pltpu.VMEM((blocks, heads * BLOCK, width), jnp.float32),
            pltpu.VMEM((blocks, heads * BLOCK, width), jnp.float32),
            pltpu.VMEM((blocks, heads * BLOCK, LEVELS * BLOCK), jnp.bfloat16),
            pltpu.VMEM((blocks, heads, BLOCK, width), jnp.bfloat16),
            pltpu.VMEM((2, 2, heads // 2, BLOCK, width), jnp.bfloat16),
            *[pltpu.VMEM((2, heads * BLOCK, 2 * BLOCK * (group + 1)), jnp.float32) for group in range(4)],
            pltpu.SemaphoreType.DMA((2, 9)),
            pltpu.SemaphoreType.DMA((2, 9)),
            pltpu.SemaphoreType.DMA((13,)),
            pltpu.SemaphoreType.DMA((13,)),
            pltpu.SemaphoreType.DMA((2,)),
        ],
        compiler_params=pltpu.CompilerParams(
            collective_id=0, has_side_effects=True, vmem_limit_bytes=60 * 1024 * 1024
        ),
        name="power_attention",
    )(
        queries,
        key_heads.reshape(1, blocks, BLOCK, width),
        value_tensor.reshape(1, blocks, BLOCK, width),
        distance_use,
        block_pick,
    )


def solution(mesh):
    placed = (
        P("head", "ctx", None),
        P("head", "ctx", None),
        P("head", "ctx", None),
        P("ctx", None),
        P("ctx", None),
    )
    return jax.shard_map(
        shards,
        mesh=mesh,
        in_specs=placed,
        out_specs=P(None, ("ctx", "head"), None),
        check_vma=False,
    )
```

```python
import functools
import math

import jax
import jax.numpy as jnp
from jax import lax
from jax.experimental import pallas as pl
from jax.experimental.pallas import tpu as pltpu
from jax.sharding import PartitionSpec as P

BLOCK = 128
LEVELS = 5
Y_COUNT = 4
FORWARD_BLOCKS = 3
Y1, Y2, Z1, Z2, Z4F, RELAY, Z4B, Y_RELAY, Y2_BACK = range(9)
X_COUNT = 4
STEP_HEADS = 2
UNROLL = 2
DIRECT, SIBLING, LEG1, LEG2 = 0, 4, 5, 9


def kernel(
    q_hbm, k_ref, v_ref, use_ref, pick_ref, out_ref,
    q_ref, far_keys, far_values, relay_ref, y_relay_ref, total_ref, inverse_ref, weight_ref, made_ref, passing_ref,
    near_0, near_1, near_2, near_3,
    send_sem, recv_sem, out_send_sem, out_recv_sem, own_sem,
):
    heads, tokens, width = q_ref.shape
    blocks = tokens // BLOCK
    ctx = lax.axis_index("ctx")
    head = lax.axis_index("head")
    shards = lax.axis_size("ctx")
    head_devices = lax.axis_size("head")
    z = ctx // Y_COUNT
    y = ctx % Y_COUNT
    along_z = lambda steps: lax.rem(ctx + (steps * Y_COUNT) % shards, shards)
    along_y = lambda steps: z * Y_COUNT + lax.rem(y + steps % Y_COUNT, Y_COUNT)

    take_queries = pltpu.make_async_copy(q_hbm, q_ref, own_sem.at[0])
    take_queries.start()

    barrier = pltpu.get_barrier_semaphore()
    ctx_peers = [along_z(s) for s in (1, -1, 2, -2, 3, -3)] + [along_y(s) for s in (1, -1)]
    for peer in ctx_peers:
        pl.semaphore_signal(barrier, inc=1, device_id={"ctx": peer}, device_id_type=pl.DeviceIdType.MESH)
    for step in range(1, head_devices):
        pl.semaphore_signal(
            barrier, inc=1, device_id={"head": lax.rem(head + step, head_devices)},
            device_id_type=pl.DeviceIdType.MESH,
        )
    pl.semaphore_wait(barrier, len(ctx_peers) + head_devices - 1)

    own = (k_ref.at[0], v_ref.at[0])
    far = (far_keys, far_values)
    near_refs = (near_0, near_1, near_2, near_3)
    top = pl.ds(0, FORWARD_BLOCKS)
    rest = pl.ds(FORWARD_BLOCKS, blocks - FORWARD_BLOCKS)

    def copy(kind, lane, source, target, peer):
        return pltpu.make_async_remote_copy(
            src_ref=source, dst_ref=target,
            send_sem=send_sem.at[kind, lane], recv_sem=recv_sem.at[kind, lane],
            device_id={"ctx": peer}, device_id_type=pl.DeviceIdType.MESH,
        )

    def near_y1(t): return copy(t, Y1, own[t], far[t].at[0], along_y(1))
    def wrap_y1(t): return copy(t, Y1, far[t].at[2], far[t].at[0], along_y(1))
    def forward_y2(t): return copy(t, Y2, far[t].at[0], far[t].at[1], along_y(1))
    def hop_y_relay(t): return copy(t, Y_RELAY, far[t].at[2], y_relay_ref.at[t], along_y(-1))
    def back_y2(t): return copy(t, Y2_BACK, y_relay_ref.at[t], far[t].at[1], along_y(-1))
    def hop_z1(t): return copy(t, Z1, own[t], far[t].at[2], along_z(1))
    def hop_z2(t): return copy(t, Z2, far[t].at[2], far[t].at[3], along_z(1))
    def hop_z4f(t): return copy(t, Z4F, far[t].at[3, top], far[t].at[4, top], along_z(2))
    def hop_relay(t): return copy(t, RELAY, own[t].at[rest], relay_ref.at[t], along_z(-3))
    def hop_z4b(t): return copy(t, Z4B, relay_ref.at[t], far[t].at[4, rest], along_z(-1))

    relays = (z >= 5) | (z == 0)
    forwards = (z >= 2) & (z <= 5)

    def first(t):
        pl.when(z < 7)(lambda: hop_z1(t).start())
        pl.when(z < 4)(lambda: hop_relay(t).start())
        pl.when(y < 3)(lambda: near_y1(t).start())

    def second(t):
        @pl.when(z >= 1)
        def _():
            hop_z1(t).wait_recv()
            pl.when(z <= 6)(lambda: hop_z2(t).start())
            pl.when(y == 3)(lambda: wrap_y1(t).start())
            pl.when(y == 2)(lambda: hop_y_relay(t).start())

        @pl.when((y == 1) | (y == 2))
        def _():
            near_y1(t).wait_recv()
            forward_y2(t).start()

    def third(t):
        pl.when(z >= 2)(lambda: hop_z2(t).wait_recv())
        pl.when(forwards)(lambda: hop_z4f(t).start())

    def fourth(t):
        @pl.when((y == 0) & (z >= 1))
        def _():
            near_y1(t).wait_recv()
            forward_y2(t).start()

        @pl.when((y == 1) & (z >= 1))
        def _():
            hop_y_relay(t).wait_recv()
            back_y2(t).start()

        @pl.when(relays)
        def _():
            hop_relay(t).wait_recv()
            hop_z4b(t).start()

    def last(t):
        pl.when(y == 3)(lambda: near_y1(t).wait_recv())
        pl.when((y >= 2) | ((y == 1) & (z >= 1)))(lambda: forward_y2(t).wait_recv())
        pl.when((y == 0) & (z >= 1))(lambda: back_y2(t).wait_recv())

        @pl.when(z >= 4)
        def _():
            hop_z4f(t).wait_recv()
            hop_z4b(t).wait_recv()

    def all_sent(t):
        pl.when(z < 7)(lambda: hop_z1(t).wait_send())
        pl.when(z < 4)(lambda: hop_relay(t).wait_send())
        pl.when((y < 3) | (z >= 1))(lambda: near_y1(t).wait_send())
        pl.when((y == 1) | (y == 2) | ((y == 0) & (z >= 1)))(lambda: forward_y2(t).wait_send())
        pl.when((y == 2) & (z >= 1))(lambda: hop_y_relay(t).wait_send())
        pl.when((y == 1) & (z >= 1))(lambda: back_y2(t).wait_send())
        pl.when((z >= 1) & (z <= 6))(lambda: hop_z2(t).wait_send())
        pl.when(forwards)(lambda: hop_z4f(t).wait_send())
        pl.when(relays)(lambda: hop_z4b(t).wait_send())

    first(0)
    for level in range(LEVELS):
        @pl.when(ctx < 2**level)
        def _(level=level):
            nothing = jnp.zeros((blocks, BLOCK, width), far_keys.dtype)
            far_keys[level] = nothing
            far_values[level] = nothing

    take_queries.wait()

    def picked(t, block):
        return jnp.concatenate(
            [far[t][level, pick_ref[block, level]] for level in range(LEVELS)], axis=0
        )

    exponent_scale = math.log2(math.e) / math.sqrt(width)
    bias = []
    for level in range(LEVELS):
        live = use_ref[0, level] * jnp.where(ctx >= 2**level, 1, 0)
        bias.append(jnp.full((1, BLOCK), (live.astype(jnp.float32) - 1.0) * 3e38, jnp.float32))
    bias = jnp.concatenate(bias, axis=1)
    rows = 2 * BLOCK
    step_rows = STEP_HEADS * BLOCK
    steps_per_block = heads // STEP_HEADS

    def group_shape(group):
        before = group * 2 * BLOCK
        return before, before + 2 * BLOCK

    def place_of(step, group):
        in_group = step // steps_per_block
        part = step % steps_per_block
        block = group * 2 + in_group
        first_row = pl.multiple_of(block * BLOCK, BLOCK)
        row_slice = pl.ds(pl.multiple_of(part * step_rows, step_rows), step_rows)
        q_now = q_ref[pl.ds(part * STEP_HEADS, STEP_HEADS), pl.ds(first_row, BLOCK), :]
        return in_group, block, row_slice, q_now.reshape(step_rows, width)

    def lane_peak(scores):
        return functools.reduce(
            jnp.maximum, [scores[:, c : c + BLOCK] for c in range(0, scores.shape[1], BLOCK)]
        )

    def score_near(group):
        before, near_width = group_shape(group)

        def body(step, carry):
            in_group, block, row_slice, q_now = place_of(step, group)
            keys = k_ref[0, : near_width // BLOCK].reshape(near_width, width)
            scores = lax.dot_general(
                q_now, keys, (((1,), (1,)), ((), ())), preferred_element_type=jnp.float32
            )
            row_pos = lax.broadcasted_iota(jnp.int32, (step_rows, rows), 0) % BLOCK + in_group * BLOCK
            col_pos = lax.broadcasted_iota(jnp.int32, (step_rows, rows), 1)
            diagonal = jnp.where(col_pos <= row_pos, scores[:, before:], -jnp.inf)
            parts = [scores[:, :before]] if group else []
            scores = jnp.concatenate(parts + [diagonal], axis=1)
            near_refs[group][in_group, row_slice, :] = scores
            inverse_ref[block, row_slice, :] = lane_peak(scores)
            return carry

        lax.fori_loop(0, 2 * steps_per_block, body, 0, unroll=UNROLL)

    def score_far(group):
        _, near_width = group_shape(group)

        def body(step, carry):
            in_group, block, row_slice, q_now = place_of(step, group)
            distant = lax.dot_general(
                q_now, picked(0, block), (((1,), (1,)), ((), ())), preferred_element_type=jnp.float32
            ) + bias
            peak = jnp.max(
                jnp.maximum(inverse_ref[block, row_slice, :], lane_peak(distant)), axis=1, keepdims=True
            )
            near_weights = jnp.exp2((near_refs[group][in_group, row_slice, :] - peak) * exponent_scale)
            far_weights = jnp.exp2((distant - peak) * exponent_scale)
            row_total = jnp.sum(near_weights, axis=1, keepdims=True) + jnp.sum(
                far_weights, axis=1, keepdims=True
            )
            weight_ref[block, row_slice, :] = far_weights.astype(jnp.bfloat16)
            total_ref[block, row_slice, :] = jnp.dot(
                near_weights.astype(jnp.bfloat16),
                v_ref[0, : near_width // BLOCK].reshape(near_width, width),
                preferred_element_type=jnp.float32,
            )
            inverse_ref[block, row_slice, :] = jnp.broadcast_to(1.0 / row_total, (step_rows, width))
            return carry

        lax.fori_loop(0, 2 * steps_per_block, body, 0, unroll=UNROLL)

    score_near(0)
    score_near(1)
    second(0)
    score_near(2)
    score_near(3)
    third(0)
    fourth(0)
    first(1)
    last(0)

    score_far(0)
    score_far(1)
    second(1)
    score_far(2)
    third(1)
    fourth(1)
    score_far(3)
    last(1)

    x = head // 2
    core = head % 2
    half = heads // 2

    def device(x_steps, to_core):
        return lax.rem(x + x_steps, X_COUNT) * 2 + to_core

    targets = [device(2, 0), device(2, 1), device(1, 0), device(3, 0), device(1, 1), device(3, 1), device(0, 1 - core), head]

    def make(slot):
        block = targets[slot]
        values = picked(1, block)

        def body(pair, carry):
            row_slice = pl.ds(pl.multiple_of(pair * rows, rows), rows)
            distant = jnp.dot(weight_ref[block, row_slice, :], values, preferred_element_type=jnp.float32)
            result = (total_ref[block, row_slice, :] + distant) * inverse_ref[block, row_slice, :]
            made_ref[slot, pl.ds(pair * 2, 2)] = result.astype(made_ref.dtype).reshape(2, BLOCK, width)
            return carry

        lax.fori_loop(0, heads // 2, body, 0)

    def give(source, target, sent, received, to_head):
        return pltpu.make_async_remote_copy(
            src_ref=source, dst_ref=target,
            send_sem=out_send_sem.at[sent], recv_sem=out_recv_sem.at[received],
            device_id={"head": to_head}, device_id_type=pl.DeviceIdType.MESH,
        )

    mine = pl.ds(head * heads, heads)

    def leg1(part, to_core):
        source = made_ref.at[to_core, pl.ds(part * half, half)]
        place = LEG1 + part * 2 + to_core
        return give(source, passing_ref.at[part, to_core], place, place, device((1, 3)[part], core))

    def leg2(part, to_core, received):
        source_head = device((3, 1)[part], core)
        target = out_ref.at[pl.ds(source_head * heads + part * half, half)]
        return give(
            passing_ref.at[part, to_core], target, LEG2 + part * 2 + to_core, received,
            device((1, 3)[part], to_core),
        )

    def direct(slot, received):
        return give(made_ref.at[slot], out_ref.at[mine], DIRECT + slot - 2, received, targets[slot])

    def start(slot):
        if slot < 2:
            leg1(0, slot).start()
            leg1(1, slot).start()
        elif slot < 6:
            direct(slot, DIRECT + (slot % 2) * 2 + core).start()
        else:
            direct(slot, SIBLING).start()

    for slot in range(8):
        make(slot)
        if slot:
            start(slot - 1)
    keep = pltpu.make_async_copy(made_ref.at[7], out_ref.at[mine], own_sem.at[1])
    keep.start()
    for part in range(2):
        for to_core in range(2):
            leg1(part, to_core).wait_recv()
            leg2(part, to_core, LEG2 + part * 2 + core).start()
    all_sent(0)
    all_sent(1)
    keep.wait()
    for slot in range(2, 7):
        direct(slot, DIRECT + slot - 2).wait()
    for part in range(2):
        for to_core in range(2):
            leg1(part, to_core).wait_send()
            leg2(part, to_core, LEG2 + part * 2 + to_core).wait()


def shards(queries, key_heads, value_tensor, distance_use, block_pick):
    heads, tokens, width = queries.shape
    blocks = tokens // BLOCK
    head_devices = lax.axis_size("head")
    vmem = pl.BlockSpec(memory_space=pltpu.VMEM)
    smem = pl.BlockSpec(memory_space=pltpu.SMEM)
    anywhere = pl.BlockSpec(memory_space=pl.ANY)
    return pl.pallas_call(
        kernel,
        out_shape=jax.ShapeDtypeStruct((heads * head_devices, tokens // head_devices, width), queries.dtype),
        in_specs=[anywhere, vmem, vmem, smem, smem],
        out_specs=anywhere,
        scratch_shapes=[
            pltpu.VMEM((heads, tokens, width), jnp.bfloat16),
            pltpu.VMEM((LEVELS, blocks, BLOCK, width), jnp.bfloat16),
            pltpu.VMEM((LEVELS, blocks, BLOCK, width), jnp.bfloat16),
            pltpu.VMEM((2, blocks - FORWARD_BLOCKS, BLOCK, width), jnp.bfloat16),
            pltpu.VMEM((2, blocks, BLOCK, width), jnp.bfloat16),
            pltpu.VMEM((blocks, heads * BLOCK, width), jnp.float32),
            pltpu.VMEM((blocks, heads * BLOCK, width), jnp.float32),
            pltpu.VMEM((blocks, heads * BLOCK, LEVELS * BLOCK), jnp.bfloat16),
            pltpu.VMEM((blocks, heads, BLOCK, width), jnp.bfloat16),
            pltpu.VMEM((2, 2, heads // 2, BLOCK, width), jnp.bfloat16),
            *[pltpu.VMEM((2, heads * BLOCK, 2 * BLOCK * (group + 1)), jnp.float32) for group in range(4)],
            pltpu.SemaphoreType.DMA((2, 9)),
            pltpu.SemaphoreType.DMA((2, 9)),
            pltpu.SemaphoreType.DMA((13,)),
            pltpu.SemaphoreType.DMA((13,)),
            pltpu.SemaphoreType.DMA((2,)),
        ],
        compiler_params=pltpu.CompilerParams(
            collective_id=0, has_side_effects=True, vmem_limit_bytes=60 * 1024 * 1024
        ),
        name="power_attention",
    )(
        queries,
        key_heads.reshape(1, blocks, BLOCK, width),
        value_tensor.reshape(1, blocks, BLOCK, width),
        distance_use,
        block_pick,
    )


def solution(mesh):
    placed = (
        P("head", "ctx", None),
        P("head", "ctx", None),
        P("head", "ctx", None),
        P("ctx", None),
        P("ctx", None),
    )
    return jax.shard_map(
        shards,
        mesh=mesh,
        in_specs=placed,
        out_specs=P(None, ("ctx", "head"), None),
        check_vma=False,
    )
```
